32 devices in a mesh: gx: 4 (over z), gy: 2 (over x), gz: 4 (over y, core).
Axes of the slice: x: 2, y: 2, z: 4, core: 2. Of those that a mesh axis runs over, the one named last changes fastest.
Arguments:
- right_side: float32 [4, 2, 8, 128], P('gx', 'gy', 'gz'), may hold values from -8 to 8
- diag_blocks: float32 [4, 2, 8, 128, 128], P('gx', 'gy', 'gz'), may hold values from -0.035 to 2.04, as said below
- couplings: float32 [3, 4, 2, 8, 128, 128], P(None, 'gx', 'gy', 'gz'), may hold values from -0.04 to 0.04
- pattern: int32 [3, 4, 2, 8], P(None, 'gx', 'gy', 'gz'), may hold values 0 or 1
- deflation: float32 [4, 2, 8, 32, 128], P('gx', 'gy', 'gz'), may hold values from -5 to 5
Outputs:
- solution: float32 [4, 2, 8, 128], P('gx', 'gy', 'gz')
- residual: float32 [4, 2, 8, 128], P('gx', 'gy', 'gz')
The draws below stay inside these ranges and needn't reach their ends.
Inputs may be any that keep to these rules, and one draw needn't show every extreme that they name: `diag_blocks`: each diagonal block is symmetric.
All inputs are finite; a program needn't handle non-finite values. No bound on the sum of `pattern` on one device may be relied on, other than what follows from the above.
Results may differ from the reference program's by a relative error of at most 0.00035.
Values sent between devices are 32-bit elements; how exact they have to be, the bound alone decides.
A program may use at most 64 MiB of HBM per device.

```python
import math
import jax
import jax.numpy as jnp
from jax import lax

BLOCK = 128
DEFL = 32
ITERS = 3
NBX = 4
NBY = 2
NBZ = 8


def deflation_basis(key):
    drawn = jax.random.normal(jax.random.fold_in(key, 101), (NBX, NBY, NBZ, DEFL, BLOCK), jnp.float32)
    return jnp.clip(drawn, -5.0, 5.0)


def draw_deflation(key, part):
    return deflation_basis(key)


def draw_right_side(key, part):
    basis = deflation_basis(key)
    mixing = jnp.clip(jax.random.normal(jax.random.fold_in(key, 102), (DEFL,), jnp.float32), -4.0, 4.0) * 0.25
    extent_all = (NBX, NBY, NBZ, BLOCK)
    jitter = jnp.clip(jax.random.normal(jax.random.fold_in(key, 103), extent_all, jnp.float32), -4.0, 4.0)
    combined = jitter + jnp.einsum('a,xyzak->xyzk', mixing, basis)
    return jnp.clip(combined, -8.0, 8.0)


def draw_diag_blocks(key, part):
    extent_all = (NBX, NBY, NBZ, BLOCK, BLOCK)
    jitter = jnp.clip(jax.random.normal(jax.random.fold_in(key, 201), extent_all, jnp.float32) * 0.006, -0.024, 0.024)
    mirrored = (jitter + jnp.swapaxes(jitter, -1, -2)) * 0.7071
    levels = jnp.exp(jax.random.uniform(jax.random.fold_in(key, 202), (NBX, NBY, NBZ, BLOCK), jnp.float32, 0.0, math.log(2.0)))
    identity = jnp.eye(BLOCK, dtype=jnp.float32)
    return mirrored + levels[..., None] * identity


def draw_couplings(key, part):
    extent_all = (3, NBX, NBY, NBZ, BLOCK, BLOCK)
    return jnp.clip(jax.random.normal(jax.random.fold_in(key, 301), extent_all, jnp.float32) * 0.01, -0.04, 0.04)


def touch_ends(entries, own_key, least, largest):
    index_at = [jax.random.randint(jax.random.fold_in(own_key, axis), (), 0, length) for axis, length in enumerate(entries.shape)]
    widest = entries.shape.index(max(entries.shape))
    next_to = index_at[:widest] + [(index_at[widest] + 1) % entries.shape[widest]] + index_at[widest + 1:]
    return entries.at[tuple(index_at)].set(least).at[tuple(next_to)].set(largest)


def setup_inputs(seed: int = 0) -> dict:
    arg_keys = jax.random.split(jax.random.key(seed), 6)
    return {
        "right_side": draw_right_side(jax.random.fold_in(arg_keys[5], 71), 0),
        "diag_blocks": draw_diag_blocks(jax.random.fold_in(arg_keys[5], 71), 0),
        "couplings": draw_couplings(jax.random.fold_in(arg_keys[5], 71), 0),
        "pattern": touch_ends((jax.random.randint(arg_keys[3], (3, NBX, NBY, NBZ), 0, 4) < 3).astype(jnp.int32), jax.random.fold_in(arg_keys[3], 1), 0, 1),
        "deflation": draw_deflation(jax.random.fold_in(arg_keys[5], 71), 0),
    }


HIGHEST = lax.Precision.HIGHEST

def rows_times(blocks, vectors):
    return jnp.einsum('xyzrk,xyzck->xyzcr', blocks, vectors, precision=HIGHEST)

def cols_times(blocks, vectors):
    return jnp.einsum('xyzkr,xyzck->xyzcr', blocks, vectors, precision=HIGHEST)

def toward_low(vectors, axis_num):
    extent = vectors.shape[axis_num]
    upper = lax.slice_in_dim(vectors, 1, extent, axis=axis_num)
    zeros_face = jnp.zeros_like(lax.slice_in_dim(vectors, 0, 1, axis=axis_num))
    return jnp.concatenate([upper, zeros_face], axis=axis_num)

def toward_high(vectors, axis_num):
    extent = vectors.shape[axis_num]
    lower = lax.slice_in_dim(vectors, 0, extent - 1, axis=axis_num)
    zeros_face = jnp.zeros_like(lax.slice_in_dim(vectors, 0, 1, axis=axis_num))
    return jnp.concatenate([zeros_face, lower], axis=axis_num)

def operate(diag_blocks, couplings, weights, vectors):
    accum_sum = rows_times(diag_blocks, vectors)
    for axis_num in range(3):
        coupled = couplings[axis_num]
        gate_w = weights[axis_num][:, :, :, None, None]
        accum_sum = accum_sum + gate_w * rows_times(coupled, toward_low(vectors, axis_num))
        accum_sum = accum_sum + toward_high(gate_w * cols_times(coupled, vectors), axis_num)
    return accum_sum

def spread(coarse_coef, basis):
    return jnp.einsum('a,xyzak->xyzk', coarse_coef, basis, precision=HIGHEST)

def reference(right_side, diag_blocks, couplings, pattern, deflation):
    weights = pattern.astype(jnp.float32)
    applied = operate(diag_blocks, couplings, weights, deflation)
    coarse_mat = jnp.einsum('xyzak,xyzbk->ab', deflation, applied, precision=HIGHEST)
    coarse_mat = 0.5 * (coarse_mat + coarse_mat.T)
    factor = jnp.linalg.cholesky(coarse_mat)
    projected = jnp.einsum('xyzak,xyzk->a', deflation, right_side, precision=HIGHEST)
    coarse_coef = jax.scipy.linalg.cho_solve((factor, True), projected)
    solution = spread(coarse_coef, deflation)
    residual = right_side - spread(coarse_coef, applied)
    norm_sq = jnp.sum(residual * residual)
    projected = jnp.einsum('xyzak,xyzk->a', applied, residual, precision=HIGHEST)
    coarse_coef = jax.scipy.linalg.cho_solve((factor, True), projected)
    direction = residual - spread(coarse_coef, deflation)
    for iteration in range(ITERS):
        images = operate(diag_blocks, couplings, weights, direction[:, :, :, None, :])[:, :, :, 0, :]
        step_len = norm_sq / jnp.sum(direction * images)
        solution = solution + step_len * direction
        residual = residual - step_len * images
        if iteration + 1 < ITERS:
            norm_new = jnp.sum(residual * residual)
            projected = jnp.einsum('xyzak,xyzk->a', applied, residual, precision=HIGHEST)
            coarse_coef = jax.scipy.linalg.cho_solve((factor, True), projected)
            direction = residual + norm_new / norm_sq * direction - spread(coarse_coef, deflation)
            norm_sq = norm_new
    return (solution, residual)
```

```python
import functools
import math

import jax
import jax.numpy as jnp
from jax import lax
from jax.experimental import pallas as pl
from jax.experimental.pallas import tpu as pltpu
from jax.sharding import PartitionSpec as P

ITERS = 3
AXES = ("gx", "gy", "gz")
COARSE_GROUPS = (("gy", "gz"), ("gx",))
DOT_GROUPS = (("gx", "gy", "gz"),)
MESH = pl.DeviceIdType.MESH
F32 = jnp.float32
BF16 = jnp.bfloat16


def place(index, group, sizes):
    coords = {}
    for axis in reversed(group):
        coords[axis] = lax.rem(index, sizes[axis])
        index = lax.div(index, sizes[axis])
    return coords


def position(group, sizes):
    index = 0
    for axis in group:
        index = index * sizes[axis] + lax.axis_index(axis)
    return index


def extent(group, sizes):
    return math.prod(sizes[axis] for axis in group)


def for_peers(group, sizes, action):
    count = extent(group, sizes)
    me = position(group, sizes)

    def body(k, carry):
        action(place(lax.rem(me + k, count), group, sizes))
        return carry

    lax.fori_loop(1, count, body, 0)


def split_rows(v):
    high = v.astype(BF16).astype(F32)
    rest = v - high
    middle = rest.astype(BF16).astype(F32)
    low = rest - middle
    if v.shape[0] == 1:
        row = lax.broadcasted_iota(jnp.int32, (8, v.shape[1]), 0)
        parts = jnp.where(row == 0, high, jnp.where(row == 1, middle, jnp.where(row == 2, low, 0.0)))
    else:
        parts = jnp.concatenate([high, middle, low], axis=0)
    return parts.astype(BF16)


def join_rows(out, rows):
    return out[:rows] + (out[rows : 2 * rows] + out[2 * rows : 3 * rows])


def split_pair(m):
    high = m.astype(BF16)
    return high, (m - high.astype(F32)).astype(BF16)


def times(v, high, low):
    parts = split_rows(v)
    out = jnp.dot(parts, high, preferred_element_type=F32)
    out = out + jnp.dot(parts, low, preferred_element_type=F32)
    return join_rows(out, v.shape[0])


def times_t(v, high, low):
    parts = split_rows(v)
    dims = (((1,), (1,)), ((), ()))
    out = lax.dot_general(parts, high, dims, preferred_element_type=F32)
    out = out + lax.dot_general(parts, low, dims, preferred_element_type=F32)
    return join_rows(out, v.shape[0])


def kernel(sizes, lz, block, defl, *refs):
    (right_ref, diag_ref, coup_ref, pat_ref, defl_ref, sol_ref, res_ref) = refs[:7]
    (loc_h, loc_l, out_h, out_l, in_h, in_l, zo_h, zo_l, zi_h, zi_l, proj_h, proj_l) = refs[7:19]
    n_ops = 1 + ITERS
    at = 19
    ops = []
    for _ in range(n_ops):
        ops.append(refs[at : at + 9])
        at += 9
    coarse_bufs = refs[at : at + len(COARSE_GROUPS)]
    at += len(COARSE_GROUPS)
    dot_bufs = [refs[at + k * len(DOT_GROUPS) : at + (k + 1) * len(DOT_GROUPS)] for k in range(ITERS)]
    at += ITERS * len(DOT_GROUPS)
    halo_send, halo_recv, red_send, red_recv = refs[at : at + 4]

    idx = {axis: lax.axis_index(axis) for axis in AXES}
    lower = {axis: idx[axis] > 0 for axis in AXES}
    upper = {axis: idx[axis] < sizes[axis] - 1 for axis in AXES}
    barrier = pltpu.get_barrier_semaphore()

    for op in ops:
        for ref in op[4:9]:
            ref[...] = jnp.zeros_like(ref)
        op[3][...] = jnp.zeros_like(op[3])

    def greet(peer):
        pl.semaphore_signal(barrier, inc=1, device_id=peer, device_id_type=MESH)

    for_peers(AXES, sizes, greet)

    def gate(d, c):
        return pat_ref[d, 0, 0, c].astype(F32)

    def put(ref_h, ref_l, rows, cols, value):
        high, low = split_pair(value)
        ref_h[rows, cols] = high
        ref_l[rows, cols] = low

    def span(c):
        return slice(c * block, (c + 1) * block)

    if lz > 2:
        loc_h[...] = jnp.zeros_like(loc_h)
        loc_l[...] = jnp.zeros_like(loc_l)
    for c in range(lz):
        put(loc_h, loc_l, span(c), span(c), diag_ref[0, 0, c])
        cx = gate(0, c) * coup_ref[0, 0, 0, c]
        cy = gate(1, c) * coup_ref[1, 0, 0, c]
        cz = gate(2, c) * coup_ref[2, 0, 0, c]
        put(out_h.at[c], out_l.at[c], slice(None), span(0), cx)
        put(out_h.at[c], out_l.at[c], slice(None), span(1), cy)
        put(in_h.at[c], in_l.at[c], span(0), slice(None), cx.T)
        put(in_h.at[c], in_l.at[c], span(1), slice(None), cy.T)
        if c + 1 < lz:
            put(loc_h, loc_l, span(c), span(c + 1), cz)
            put(loc_h, loc_l, span(c + 1), span(c), cz.T)
        else:
            put(zo_h, zo_l, slice(None), slice(None), cz)
            put(zi_h, zi_l, slice(None), slice(None), cz.T)

    right = jnp.concatenate([right_ref[0, 0, c : c + 1, :] for c in range(lz)], axis=1)
    basis = jnp.concatenate([defl_ref[0, 0, c] for c in range(lz)], axis=1)

    def halo_copies(k):
        field, car_x, car_y, car_z, bey_x, bey_y, bey_z, arr_xy, arr_z = ops[k]
        routes = (
            ("gx", -1, field, bey_x),
            ("gy", -1, field, bey_y),
            ("gz", -1, field.at[0], bey_z),
            ("gx", 1, car_x, arr_xy.at[0]),
            ("gy", 1, car_y, arr_xy.at[1]),
            ("gz", 1, car_z, arr_z),
        )
        copies = []
        for j, (axis, way, src, dst) in enumerate(routes):
            copies.append(
                (
                    lower[axis] if way < 0 else upper[axis],
                    upper[axis] if way < 0 else lower[axis],
                    pltpu.make_async_remote_copy(
                        src_ref=src,
                        dst_ref=dst,
                        send_sem=halo_send.at[k, j],
                        recv_sem=halo_recv.at[k, j],
                        device_id={axis: jnp.clip(idx[axis] + way, 0, sizes[axis] - 1)},
                        device_id_type=MESH,
                    ),
                )
            )
        return copies

    def start(copies):
        for sends, _, copy in copies:
            pl.when(sends)(copy.start)

    def open_product(k, v):
        field, car_x, car_y, car_z = ops[k][:4]
        copies = halo_copies(k)
        for c in range(lz):
            field[c] = v[:, span(c)]
        start(copies[:3])
        for c in range(lz):
            carried = times(v[:, span(c)], out_h[c], out_l[c])
            car_x[c] = carried[:, span(0)]
            car_y[c] = carried[:, span(1)]
        car_z[...] = times(v[:, span(lz - 1)], zo_h[...], zo_l[...])
        start(copies[3:])
        return times(v, loc_h[...], loc_l[...])

    def close_product(k, own):
        _, _, _, _, bey_x, bey_y, bey_z, arr_xy, arr_z = ops[k]
        for _, comes, copy in halo_copies(k):
            pl.when(comes)(copy.wait_recv)
        parts = []
        for c in range(lz):
            beyond = jnp.concatenate([bey_x[c], bey_y[c]], axis=1)
            part = times(beyond, in_h[c], in_l[c])
            part = part + arr_xy[0, c] + arr_xy[1, c]
            if c == 0:
                part = part + arr_z[...]
            if c == lz - 1:
                part = part + times(bey_z[...], zi_h[...], zi_l[...])
            parts.append(part)
        return own + jnp.concatenate(parts, axis=1)

    def gathered(buf, sem):
        rest = buf.at[pl.ds(0, buf.shape[0] - 1)]
        return pltpu.make_async_copy(rest, rest, sem)

    def reduce_start(buf, group, sem, value):
        me = position(group, sizes)
        buf[me] = value
        own = buf.at[me]

        def send(peer):
            pltpu.make_async_remote_copy(
                src_ref=own,
                dst_ref=own,
                send_sem=red_send.at[sem],
                recv_sem=red_recv.at[sem],
                device_id=peer,
                device_id_type=MESH,
            ).start()

        for_peers(group, sizes, send)

    def reduce_done(buf, sem):
        gathered(buf, red_recv.at[sem]).wait()
        return jnp.sum(buf[...], axis=0)

    def spread(coef, fields):
        return jnp.sum(coef * fields, axis=0, keepdims=True)

    rows_first = ops[0][0].shape[1]
    first = jnp.concatenate([basis, right, jnp.zeros((rows_first - defl - 1, lz * block), F32)], axis=0)
    pl.semaphore_wait(barrier, extent(AXES, sizes) - 1)
    own = open_product(0, first)
    proj_h[...] = jnp.zeros_like(proj_h)
    proj_l[...] = jnp.zeros_like(proj_l)
    everything = slice(None)
    put(proj_h, proj_l, slice(0, defl), everything, basis)
    right_local = times_t(right, proj_h[...], proj_l[...])
    both = close_product(0, own)
    applied = both[:defl]
    image = both[defl : defl + 1]

    reps = block // defl
    apart = defl // reps
    for g in range(reps):
        put(proj_h, proj_l, slice(g * defl, (g + 1) * defl), everything, applied)
    coarse_local = times_t(basis, proj_h[...], proj_l[...])
    lane = lax.broadcasted_iota(jnp.int32, (apart, block), 1)
    packed = jnp.zeros((apart, block), F32)
    for g in range(reps):
        inside = (lane >= g * defl) & (lane < (g + 1) * defl)
        packed = packed + jnp.where(inside, coarse_local[g * apart : (g + 1) * apart], 0.0)
    sem = 0
    value = jnp.concatenate([packed, jnp.broadcast_to(right_local, (8, block))], axis=0)
    reduce_start(coarse_bufs[0], COARSE_GROUPS[0], sem, value)
    own = open_product(1, applied)
    put(proj_h, proj_l, slice(defl, block), everything, jnp.zeros((block - defl, lz * block), F32))
    for k in range(1, len(COARSE_GROUPS)):
        value = reduce_done(coarse_bufs[k - 1], sem)
        sem += 1
        reduce_start(coarse_bufs[k], COARSE_GROUPS[k], sem, value)
    value = reduce_done(coarse_bufs[-1], sem)
    sem += 1
    coarse = jnp.concatenate(
        [value[:apart]] + [pltpu.roll(value[:apart], block - g * defl, 1) for g in range(1, reps)], axis=0
    )
    col = lax.broadcasted_iota(jnp.int32, (defl, block), 1)
    row = lax.broadcasted_iota(jnp.int32, (defl, block), 0)
    coarse = jnp.where(col < defl, coarse, 0.0)
    square = jnp.concatenate([coarse, jnp.zeros((block - defl, block), F32)], axis=0)
    inv = 0.5 * (coarse + square.T[:defl])
    for k in range(defl):
        pivot = 1.0 / inv[k : k + 1, k : k + 1]
        line = jnp.where(col[:1] == k, pivot, inv[k : k + 1] * pivot)
        inv = jnp.where(row == k, line, jnp.where(col == k, 0.0, inv) - inv[:, k : k + 1] * line)
    eye = jnp.where(row == col, 1.0, 0.0)

    def coarse_solve(projected):
        return jnp.sum(inv * projected, axis=1, keepdims=True)

    twice = close_product(1, own)
    coef = coarse_solve(value[apart : apart + 1])
    x = spread(coef, basis)
    r = right - spread(coef, applied)
    w = image - spread(coef, twice)
    d = s = z = curv = norm = None
    lane_row = lax.broadcasted_iota(jnp.int32, (1, block), 1)
    for it in range(ITERS):
        last = it + 1 == ITERS
        local = times_t(r, proj_h[...], proj_l[...])
        sq = jnp.sum(r * r, axis=1, keepdims=True)
        cross = jnp.sum(r * w, axis=1, keepdims=True)
        local = jnp.where(lane_row == defl, sq, jnp.where(lane_row == defl + 1, cross, local))
        bufs = dot_bufs[it]
        reduce_start(bufs[0], DOT_GROUPS[0], sem, local)
        if not last:
            own = open_product(2 + it, w)
        for k in range(1, len(DOT_GROUPS)):
            local = reduce_done(bufs[k - 1], sem)
            sem += 1
            reduce_start(bufs[k], DOT_GROUPS[k], sem, local)
        if not last:
            q = close_product(2 + it, own)
        total = reduce_done(bufs[-1], sem)
        sem += 1
        coef = coarse_solve(total)
        mine = jnp.sum(eye * total, axis=1, keepdims=True)
        energy = jnp.sum(mine * coef, axis=0, keepdims=True)
        norm_new = total[:, defl : defl + 1]
        cross = total[:, defl + 1 : defl + 2]
        if it == 0:
            d = r - spread(coef, basis)
            s = w - spread(coef, applied)
            z = q - spread(coef, twice)
            curv = cross - energy
        else:
            growth = norm_new / norm
            d = r + growth * d - spread(coef, basis)
            s = w + growth * s - spread(coef, applied)
            if not last:
                z = q + growth * z - spread(coef, twice)
            curv = cross - growth * growth * curv - energy
        norm = norm_new
        step = norm / curv
        x = x + step * d
        r = r - step * s
        if not last:
            w = w - step * z
    for c in range(lz):
        sol_ref[0, 0, c : c + 1, :] = x[:, span(c)]
        res_ref[0, 0, c : c + 1, :] = r[:, span(c)]

    for k in range(n_ops):
        for sends, _, copy in halo_copies(k):
            pl.when(sends)(copy.wait_send)
    every = list(coarse_bufs) + [buf for bufs in dot_bufs for buf in bufs]
    for k, buf in enumerate(every):
        gathered(buf, red_send.at[k]).wait()


def solution(mesh):
    sizes = dict(mesh.shape)
    in_specs = (
        P("gx", "gy", "gz", None),
        P("gx", "gy", "gz", None, None),
        P(None, "gx", "gy", "gz", None, None),
        P(None, "gx", "gy", "gz"),
        P("gx", "gy", "gz", None, None),
    )
    out_specs = (P("gx", "gy", "gz", None), P("gx", "gy", "gz", None))

    def per_device(right_side, diag_blocks, couplings, pattern, deflation):
        lx, ly, lz, block = right_side.shape
        assert lx == 1 and ly == 1
        defl = deflation.shape[3]
        rows_first = (defl + 1 + 7) // 8 * 8
        wide = lz * block
        scratch = []
        for shape in (
            (wide, wide),
            (lz, block, 2 * block),
            (lz, 2 * block, block),
            (block, block),
            (block, block),
            (block, wide),
        ):
            scratch += [pltpu.VMEM(shape, BF16)] * 2
        for rows in (rows_first, defl) + (1,) * (ITERS - 1):
            layer, face = (lz, rows, block), (rows, block)
            scratch += [pltpu.VMEM(layer, F32)] * 3 + [pltpu.VMEM(face, F32)]
            scratch += [pltpu.VMEM(layer, F32)] * 2 + [pltpu.VMEM(face, F32)]
            scratch += [pltpu.VMEM((2,) + layer, F32), pltpu.VMEM(face, F32)]
        for group in COARSE_GROUPS:
            scratch.append(pltpu.VMEM((extent(group, sizes), defl * defl // block + 8, block), F32))
        for _ in range(ITERS):
            for group in DOT_GROUPS:
                scratch.append(pltpu.VMEM((extent(group, sizes), 1, block), F32))
        reductions = len(COARSE_GROUPS) + ITERS * len(DOT_GROUPS)
        scratch += [pltpu.SemaphoreType.DMA((1 + ITERS, 6))] * 2
        scratch += [pltpu.SemaphoreType.DMA((reductions,))] * 2
        vmem = pl.BlockSpec(memory_space=pltpu.VMEM)
        smem = pl.BlockSpec(memory_space=pltpu.SMEM)
        out = jax.ShapeDtypeStruct(right_side.shape, F32)
        return pl.pallas_call(
            functools.partial(kernel, sizes, lz, block, defl),
            out_shape=(out, out),
            in_specs=[vmem, vmem, vmem, smem, vmem],
            out_specs=(vmem, vmem),
            scratch_shapes=scratch,
            compiler_params=pltpu.CompilerParams(
                collective_id=0, has_side_effects=True, vmem_limit_bytes=48 * 1024 * 1024
            ),
        )(right_side, diag_blocks, couplings, pattern, deflation)

    return jax.shard_map(
        per_device, mesh=mesh, in_specs=in_specs, out_specs=out_specs, check_vma=False
    )
```

```python
import functools
import math

import jax
import jax.numpy as jnp
from jax import lax
from jax.experimental import pallas as pl
from jax.experimental.pallas import tpu as pltpu
from jax.sharding import PartitionSpec as P

ITERS = 3
AXES = ("gx", "gy", "gz")
COARSE_GROUPS = (("gy", "gz"), ("gx",))
UNROLLED = 32
DOT_GROUPS = (("gx", "gy", "gz"),)
MESH = pl.DeviceIdType.MESH
F32 = jnp.float32
BF16 = jnp.bfloat16


def place(index, group, sizes):
    coords = {}
    for axis in reversed(group):
        coords[axis] = lax.rem(index, sizes[axis])
        index = lax.div(index, sizes[axis])
    return coords


def position(group, sizes):
    index = 0
    for axis in group:
        index = index * sizes[axis] + lax.axis_index(axis)
    return index


def extent(group, sizes):
    return math.prod(sizes[axis] for axis in group)


def for_peers(group, sizes, action):
    count = extent(group, sizes)
    me = position(group, sizes)

    def body(k, carry):
        action(place(lax.rem(me + k, count), group, sizes))
        return carry

    if count <= UNROLLED:
        for k in range(1, count):
            body(k, 0)
    else:
        lax.fori_loop(1, count, body, 0)


def split_rows(v):
    high = v.astype(BF16).astype(F32)
    rest = v - high
    middle = rest.astype(BF16).astype(F32)
    low = rest - middle
    if v.shape[0] == 1:
        row = lax.broadcasted_iota(jnp.int32, (8, v.shape[1]), 0)
        parts = jnp.where(row == 0, high, jnp.where(row == 1, middle, jnp.where(row == 2, low, 0.0)))
    else:
        parts = jnp.concatenate([high, middle, low], axis=0)
    return parts.astype(BF16)


def join_rows(out, rows):
    return out[:rows] + (out[rows : 2 * rows] + out[2 * rows : 3 * rows])


def split_pair(m):
    high = m.astype(BF16)
    return high, (m - high.astype(F32)).astype(BF16)


def times(v, high, low):
    parts = split_rows(v)
    out = jnp.dot(parts, high, preferred_element_type=F32)
    out = out + jnp.dot(parts, low, preferred_element_type=F32)
    return join_rows(out, v.shape[0])


def times_t(v, high, low):
    parts = split_rows(v)
    dims = (((1,), (1,)), ((), ()))
    out = lax.dot_general(parts, high, dims, preferred_element_type=F32)
    out = out + lax.dot_general(parts, low, dims, preferred_element_type=F32)
    return join_rows(out, v.shape[0])


def kernel(sizes, lz, block, defl, *refs):
    inputs = refs[:5]
    sol_ref, res_ref = refs[5:7]
    (loc_h, loc_l, out_h, out_l, in_h, in_l, zo_h, zo_l, zi_h, zi_l, proj_h, proj_l) = refs[7:19]
    n_ops = 1 + ITERS
    at = 19
    ops = []
    for _ in range(n_ops):
        ops.append(refs[at : at + 9])
        at += 9
    coarse_bufs = refs[at : at + len(COARSE_GROUPS)]
    at += len(COARSE_GROUPS)
    dot_bufs = [refs[at + k * len(DOT_GROUPS) : at + (k + 1) * len(DOT_GROUPS)] for k in range(ITERS)]
    at += ITERS * len(DOT_GROUPS)
    halo_send, halo_recv, red_send, red_recv, load_sem = refs[at : at + 5]
    staged = refs[at + 5 : at + 10]
    loads = [pltpu.make_async_copy(src, dst, load_sem.at[k]) for k, (src, dst) in enumerate(zip(inputs, staged))]
    for load in loads:
        load.start()
    right_ref, diag_ref, coup_ref, pat_ref, defl_ref = staged

    idx = {axis: lax.axis_index(axis) for axis in AXES}
    lower = {axis: idx[axis] > 0 for axis in AXES}
    upper = {axis: idx[axis] < sizes[axis] - 1 for axis in AXES}
    barrier = pltpu.get_barrier_semaphore()

    for op in ops:
        for ref in op[4:9]:
            ref[...] = jnp.zeros_like(ref)
        op[3][...] = jnp.zeros_like(op[3])

    def greet(peer):
        pl.semaphore_signal(barrier, inc=1, device_id=peer, device_id_type=MESH)

    for group in COARSE_GROUPS:
        for_peers(group, sizes, greet)
    for load in loads:
        load.wait()

    def gate(d, c):
        return pat_ref[0, 0, c : c + 1, d : d + 1].astype(F32)

    def put(ref_h, ref_l, rows, cols, value):
        high, low = split_pair(value)
        ref_h[rows, cols] = high
        ref_l[rows, cols] = low

    def span(c):
        return slice(c * block, (c + 1) * block)

    if lz > 2:
        loc_h[...] = jnp.zeros_like(loc_h)
        loc_l[...] = jnp.zeros_like(loc_l)
    for c in range(lz):
        put(loc_h, loc_l, span(c), span(c), diag_ref[0, 0, c])
        cx = gate(0, c) * coup_ref[0, 0, 0, c]
        cy = gate(1, c) * coup_ref[1, 0, 0, c]
        cz = gate(2, c) * coup_ref[2, 0, 0, c]
        put(out_h.at[c], out_l.at[c], slice(None), span(0), cx)
        put(out_h.at[c], out_l.at[c], slice(None), span(1), cy)
        put(in_h.at[c], in_l.at[c], span(0), slice(None), cx.T)
        put(in_h.at[c], in_l.at[c], span(1), slice(None), cy.T)
        if c + 1 < lz:
            put(loc_h, loc_l, span(c), span(c + 1), cz)
            put(loc_h, loc_l, span(c + 1), span(c), cz.T)
        else:
            put(zo_h, zo_l, slice(None), slice(None), cz)
            put(zi_h, zi_l, slice(None), slice(None), cz.T)

    right = jnp.concatenate([right_ref[0, 0, c : c + 1, :] for c in range(lz)], axis=1)
    basis = jnp.concatenate([defl_ref[0, 0, c] for c in range(lz)], axis=1)

    def halo_copies(k):
        field, car_x, car_y, car_z, bey_x, bey_y, bey_z, arr_xy, arr_z = ops[k]
        routes = (
            ("gx", -1, field, bey_x),
            ("gy", -1, field, bey_y),
            ("gz", -1, field.at[0], bey_z),
            ("gx", 1, car_x, arr_xy.at[0]),
            ("gy", 1, car_y, arr_xy.at[1]),
            ("gz", 1, car_z, arr_z),
        )
        copies = []
        for j, (axis, way, src, dst) in enumerate(routes):
            copies.append(
                (
                    lower[axis] if way < 0 else upper[axis],
                    upper[axis] if way < 0 else lower[axis],
                    pltpu.make_async_remote_copy(
                        src_ref=src,
                        dst_ref=dst,
                        send_sem=halo_send.at[k, j],
                        recv_sem=halo_recv.at[k, j],
                        device_id={axis: jnp.clip(idx[axis] + way, 0, sizes[axis] - 1)},
                        device_id_type=MESH,
                    ),
                )
            )
        return copies

    def start(copies):
        for sends, _, copy in copies:
            pl.when(sends)(copy.start)

    def open_product(k, v, later=None):
        field, car_x, car_y, car_z = ops[k][:4]
        copies = halo_copies(k) if later is None else None
        for c in range(lz):
            field[c] = v[:, span(c)]
        if later is None:
            start(copies[:3])
        for c in range(lz):
            carried = times(v[:, span(c)], out_h[c], out_l[c])
            car_x[c] = carried[:, span(0)]
            car_y[c] = carried[:, span(1)]
        car_z[...] = times(v[:, span(lz - 1)], zo_h[...], zo_l[...])
        if later is None:
            start(copies[3:])
        return times(v, loc_h[...], loc_l[...])

    def close_product(k, own):
        _, _, _, _, bey_x, bey_y, bey_z, arr_xy, arr_z = ops[k]
        for _, comes, copy in halo_copies(k):
            pl.when(comes)(copy.wait_recv)
        parts = []
        for c in range(lz):
            beyond = jnp.concatenate([bey_x[c], bey_y[c]], axis=1)
            part = times(beyond, in_h[c], in_l[c])
            part = part + arr_xy[0, c] + arr_xy[1, c]
            if c == 0:
                part = part + arr_z[...]
            if c == lz - 1:
                part = part + times(bey_z[...], zi_h[...], zi_l[...])
            parts.append(part)
        return own + jnp.concatenate(parts, axis=1)

    def gathered(buf, sem):
        rest = buf.at[pl.ds(0, buf.shape[0] - 1)]
        return pltpu.make_async_copy(rest, rest, sem)

    def reduce_start(buf, group, sem, value):
        me = position(group, sizes)
        buf[me] = value
        own = buf.at[me]

        def send(peer):
            pltpu.make_async_remote_copy(
                src_ref=own,
                dst_ref=own,
                send_sem=red_send.at[sem],
                recv_sem=red_recv.at[sem],
                device_id=peer,
                device_id_type=MESH,
            ).start()

        for_peers(group, sizes, send)

    def reduce_done(buf, sem):
        gathered(buf, red_recv.at[sem]).wait()
        return jnp.sum(buf[...], axis=0)

    def spread(coef, fields):
        return jnp.sum(coef * fields, axis=0, keepdims=True)

    rows_first = ops[0][0].shape[1]
    first = jnp.concatenate([basis, right, jnp.zeros((rows_first - defl - 1, lz * block), F32)], axis=0)
    pl.semaphore_wait(barrier, sum(extent(group, sizes) - 1 for group in COARSE_GROUPS))
    own = open_product(0, first)
    proj_h[...] = jnp.zeros_like(proj_h)
    proj_l[...] = jnp.zeros_like(proj_l)
    everything = slice(None)
    put(proj_h, proj_l, slice(0, defl), everything, basis)
    right_local = times_t(right, proj_h[...], proj_l[...])
    both = close_product(0, own)
    applied = both[:defl]
    image = both[defl : defl + 1]

    reps = block // defl
    apart = defl // reps
    for g in range(reps):
        put(proj_h, proj_l, slice(g * defl, (g + 1) * defl), everything, applied)
    coarse_local = times_t(basis, proj_h[...], proj_l[...])
    lane = lax.broadcasted_iota(jnp.int32, (apart, block), 1)
    packed = jnp.zeros((apart, block), F32)
    for g in range(reps):
        inside = (lane >= g * defl) & (lane < (g + 1) * defl)
        packed = packed + jnp.where(inside, coarse_local[g * apart : (g + 1) * apart], 0.0)
    sem = 0
    value = jnp.concatenate([packed, jnp.broadcast_to(right_local, (8, block))], axis=0)
    reduce_start(coarse_bufs[0], COARSE_GROUPS[0], sem, value)
    own = open_product(1, applied, "later")
    put(proj_h, proj_l, slice(defl, block), everything, jnp.zeros((block - defl, lz * block), F32))
    for k in range(1, len(COARSE_GROUPS)):
        value = reduce_done(coarse_bufs[k - 1], sem)
        sem += 1
        reduce_start(coarse_bufs[k], COARSE_GROUPS[k], sem, value)
    start(halo_copies(1))
    value = reduce_done(coarse_bufs[-1], sem)
    sem += 1
    coarse = jnp.concatenate(
        [value[:apart]] + [pltpu.roll(value[:apart], block - g * defl, 1) for g in range(1, reps)], axis=0
    )
    col = lax.broadcasted_iota(jnp.int32, (defl, block), 1)
    row = lax.broadcasted_iota(jnp.int32, (defl, block), 0)
    coarse = jnp.where(col < defl, coarse, 0.0)
    square = jnp.concatenate([coarse, jnp.zeros((block - defl, block), F32)], axis=0)
    inv = 0.5 * (coarse + square.T[:defl])
    for k in range(defl):
        pivot = 1.0 / inv[k : k + 1, k : k + 1]
        line = jnp.where(col[:1] == k, pivot, inv[k : k + 1] * pivot)
        inv = jnp.where(row == k, line, jnp.where(col == k, 0.0, inv) - inv[:, k : k + 1] * line)
    eye = jnp.where(row == col, 1.0, 0.0)

    def coarse_solve(projected):
        return jnp.sum(inv * projected, axis=1, keepdims=True)

    twice = close_product(1, own)
    coef = coarse_solve(value[apart : apart + 1])
    x = spread(coef, basis)
    r = right - spread(coef, applied)
    w = image - spread(coef, twice)
    d = s = z = curv = norm = None
    lane_row = lax.broadcasted_iota(jnp.int32, (1, block), 1)
    for it in range(ITERS):
        last = it + 1 == ITERS
        local = times_t(r, proj_h[...], proj_l[...])
        sq = jnp.sum(r * r, axis=1, keepdims=True)
        cross = jnp.sum(r * w, axis=1, keepdims=True)
        local = jnp.where(lane_row == defl, sq, jnp.where(lane_row == defl + 1, cross, local))
        bufs = dot_bufs[it]
        reduce_start(bufs[0], DOT_GROUPS[0], sem, local)
        if not last:
            own = open_product(2 + it, w)
        for k in range(1, len(DOT_GROUPS)):
            local = reduce_done(bufs[k - 1], sem)
            sem += 1
            reduce_start(bufs[k], DOT_GROUPS[k], sem, local)
        if not last:
            q = close_product(2 + it, own)
        total = reduce_done(bufs[-1], sem)
        sem += 1
        coef = coarse_solve(total)
        mine = jnp.sum(eye * total, axis=1, keepdims=True)
        energy = jnp.sum(mine * coef, axis=0, keepdims=True)
        norm_new = total[:, defl : defl + 1]
        cross = total[:, defl + 1 : defl + 2]
        if it == 0:
            d = r - spread(coef, basis)
            s = w - spread(coef, applied)
            z = q - spread(coef, twice)
            curv = cross - energy
        else:
            growth = norm_new / norm
            d = r + growth * d - spread(coef, basis)
            s = w + growth * s - spread(coef, applied)
            if not last:
                z = q + growth * z - spread(coef, twice)
            curv = cross - growth * growth * curv - energy
        norm = norm_new
        step = norm / curv
        x = x + step * d
        r = r - step * s
        if not last:
            w = w - step * z
    for c in range(lz):
        sol_ref[0, 0, c : c + 1, :] = x[:, span(c)]
        res_ref[0, 0, c : c + 1, :] = r[:, span(c)]

    for k in range(n_ops):
        for sends, _, copy in halo_copies(k):
            pl.when(sends)(copy.wait_send)
    every = list(coarse_bufs) + [buf for bufs in dot_bufs for buf in bufs]
    for k, buf in enumerate(every):
        gathered(buf, red_send.at[k]).wait()


def hand_out(sol_ref, res_ref, sol_out, res_out, sems):
    copies = [
        pltpu.make_async_copy(sol_ref, sol_out, sems.at[0]),
        pltpu.make_async_copy(res_ref, res_out, sems.at[1]),
    ]
    for copy in copies:
        copy.start()
    for copy in copies:
        copy.wait()


def solution(mesh):
    sizes = dict(mesh.shape)
    in_specs = (
        P("gx", "gy", "gz", None),
        P("gx", "gy", "gz", None, None),
        P(None, "gx", "gy", "gz", None, None),
        P(None, "gx", "gy", "gz"),
        P("gx", "gy", "gz", None, None),
    )
    out_specs = (P("gx", "gy", "gz", None), P("gx", "gy", "gz", None))

    def per_device(right_side, diag_blocks, couplings, pattern, deflation):
        lx, ly, lz, block = right_side.shape
        pattern = jnp.transpose(pattern, (1, 2, 3, 0))
        assert lx == 1 and ly == 1
        defl = deflation.shape[3]
        rows_first = (defl + 1 + 7) // 8 * 8
        wide = lz * block
        scratch = []
        for shape in (
            (wide, wide),
            (lz, block, 2 * block),
            (lz, 2 * block, block),
            (block, block),
            (block, block),
            (block, wide),
        ):
            scratch += [pltpu.VMEM(shape, BF16)] * 2
        for rows in (rows_first, defl) + (1,) * (ITERS - 1):
            layer, face = (lz, rows, block), (rows, block)
            scratch += [pltpu.VMEM(layer, F32)] * 3 + [pltpu.VMEM(face, F32)]
            scratch += [pltpu.VMEM(layer, F32)] * 2 + [pltpu.VMEM(face, F32)]
            scratch += [pltpu.VMEM((2,) + layer, F32), pltpu.VMEM(face, F32)]
        for group in COARSE_GROUPS:
            scratch.append(pltpu.VMEM((extent(group, sizes), defl * defl // block + 8, block), F32))
        for _ in range(ITERS):
            for group in DOT_GROUPS:
                scratch.append(pltpu.VMEM((extent(group, sizes), 1, block), F32))
        reductions = len(COARSE_GROUPS) + ITERS * len(DOT_GROUPS)
        scratch += [pltpu.SemaphoreType.DMA((1 + ITERS, 6))] * 2
        scratch += [pltpu.SemaphoreType.DMA((reductions,))] * 2
        scratch.append(pltpu.SemaphoreType.DMA((5,)))
        for array in (right_side, diag_blocks, couplings, pattern, deflation):
            scratch.append(pltpu.VMEM(array.shape, array.dtype))
        vmem = pl.BlockSpec(memory_space=pltpu.VMEM)
        anywhere = pl.BlockSpec(memory_space=pl.ANY)
        out = jax.ShapeDtypeStruct(right_side.shape, F32)
        results = pl.pallas_call(
            functools.partial(kernel, sizes, lz, block, defl),
            out_shape=(out, out),
            in_specs=[anywhere] * 5,
            out_specs=(vmem, vmem),
            scratch_shapes=scratch,
            compiler_params=pltpu.CompilerParams(
                collective_id=0, has_side_effects=True, vmem_limit_bytes=48 * 1024 * 1024
            ),
        )(right_side, diag_blocks, couplings, pattern, deflation)
        return pl.pallas_call(
            hand_out,
            out_shape=(out, out),
            in_specs=[vmem, vmem],
            out_specs=(anywhere, anywhere),
            scratch_shapes=[pltpu.SemaphoreType.DMA((2,))],
        )(*results)

    return jax.shard_map(
        per_device, mesh=mesh, in_specs=in_specs, out_specs=out_specs, check_vma=False
    )
```

```python
import functools
import math

import jax
import jax.numpy as jnp
from jax import lax
from jax.experimental import pallas as pl
from jax.experimental.pallas import tpu as pltpu
from jax.sharding import PartitionSpec as P

ITERS = 3
AXES = ("gx", "gy", "gz")
COARSE_GROUPS = (("gy", "gz"), ("gx",))
UNROLLED = 32
DOT_GROUPS = (("gx", "gy", "gz"),)
MESH = pl.DeviceIdType.MESH
F32 = jnp.float32
BF16 = jnp.bfloat16


def place(index, group, sizes):
    coords = {}
    for axis in reversed(group):
        coords[axis] = lax.rem(index, sizes[axis])
        index = lax.div(index, sizes[axis])
    return coords


def position(group, sizes):
    index = 0
    for axis in group:
        index = index * sizes[axis] + lax.axis_index(axis)
    return index


def extent(group, sizes):
    return math.prod(sizes[axis] for axis in group)


def for_peers(group, sizes, action):
    count = extent(group, sizes)
    me = position(group, sizes)

    def body(k, carry):
        action(place(lax.rem(me + k, count), group, sizes))
        return carry

    if count <= UNROLLED:
        for k in range(1, count):
            body(k, 0)
    else:
        lax.fori_loop(1, count, body, 0)


def split_rows(v):
    high = v.astype(BF16).astype(F32)
    rest = v - high
    middle = rest.astype(BF16).astype(F32)
    low = rest - middle
    if v.shape[0] == 1:
        row = lax.broadcasted_iota(jnp.int32, (8, v.shape[1]), 0)
        parts = jnp.where(row == 0, high, jnp.where(row == 1, middle, jnp.where(row == 2, low, 0.0)))
    else:
        parts = jnp.concatenate([high, middle, low], axis=0)
    return parts.astype(BF16)


def join_rows(out, rows):
    return out[:rows] + (out[rows : 2 * rows] + out[2 * rows : 3 * rows])


def split_pair(m):
    high = m.astype(BF16)
    return high, (m - high.astype(F32)).astype(BF16)


def times(v, high, low):
    parts = split_rows(v)
    out = jnp.dot(parts, high, preferred_element_type=F32)
    out = out + jnp.dot(parts, low, preferred_element_type=F32)
    return join_rows(out, v.shape[0])


def times_t(v, high, low):
    parts = split_rows(v)
    dims = (((1,), (1,)), ((), ()))
    out = lax.dot_general(parts, high, dims, preferred_element_type=F32)
    out = out + lax.dot_general(parts, low, dims, preferred_element_type=F32)
    return join_rows(out, v.shape[0])


def kernel(sizes, lz, block, defl, *refs):
    inputs = refs[:5]
    sol_ref, res_ref = refs[5:7]
    (loc_h, loc_l, out_h, out_l, in_h, in_l, zo_h, zo_l, zi_h, zi_l, proj_h, proj_l) = refs[7:19]
    n_ops = 1 + ITERS
    at = 19
    ops = []
    for _ in range(n_ops):
        ops.append(refs[at : at + 9])
        at += 9
    coarse_bufs = refs[at : at + len(COARSE_GROUPS)]
    at += len(COARSE_GROUPS)
    dot_bufs = [refs[at + k * len(DOT_GROUPS) : at + (k + 1) * len(DOT_GROUPS)] for k in range(ITERS)]
    at += ITERS * len(DOT_GROUPS)
    halo_send, halo_recv, red_send, red_recv, load_sem = refs[at : at + 5]
    staged = refs[at + 5 : at + 10]
    loads = [pltpu.make_async_copy(src, dst, load_sem.at[k]) for k, (src, dst) in enumerate(zip(inputs, staged))]
    for load in loads:
        load.start()
    right_ref, diag_ref, coup_ref, pat_ref, defl_ref = staged

    idx = {axis: lax.axis_index(axis) for axis in AXES}
    lower = {axis: idx[axis] > 0 for axis in AXES}
    upper = {axis: idx[axis] < sizes[axis] - 1 for axis in AXES}
    barrier = pltpu.get_barrier_semaphore()

    for op in ops:
        for ref in op[4:9]:
            ref[...] = jnp.zeros_like(ref)
        op[3][...] = jnp.zeros_like(op[3])

    def greet(peer):
        pl.semaphore_signal(barrier, inc=1, device_id=peer, device_id_type=MESH)

    for group in COARSE_GROUPS:
        for_peers(group, sizes, greet)
    for load in loads:
        load.wait()

    def gate(d, c):
        return pat_ref[0, 0, c : c + 1, d : d + 1].astype(F32)

    def put(ref_h, ref_l, rows, cols, value):
        high, low = split_pair(value)
        ref_h[rows, cols] = high
        ref_l[rows, cols] = low

    def span(c):
        return slice(c * block, (c + 1) * block)

    if lz > 2:
        loc_h[...] = jnp.zeros_like(loc_h)
        loc_l[...] = jnp.zeros_like(loc_l)
    for c in range(lz):
        put(loc_h, loc_l, span(c), span(c), diag_ref[0, 0, c])
        cx = gate(0, c) * coup_ref[0, 0, 0, c]
        cy = gate(1, c) * coup_ref[1, 0, 0, c]
        cz = gate(2, c) * coup_ref[2, 0, 0, c]
        put(out_h.at[c], out_l.at[c], slice(None), span(0), cx)
        put(out_h.at[c], out_l.at[c], slice(None), span(1), cy)
        put(in_h.at[c], in_l.at[c], span(0), slice(None), cx.T)
        put(in_h.at[c], in_l.at[c], span(1), slice(None), cy.T)
        if c + 1 < lz:
            put(loc_h, loc_l, span(c), span(c + 1), cz)
            put(loc_h, loc_l, span(c + 1), span(c), cz.T)
        else:
            put(zo_h, zo_l, slice(None), slice(None), cz)
            put(zi_h, zi_l, slice(None), slice(None), cz.T)

    right = jnp.concatenate([right_ref[0, 0, c : c + 1, :] for c in range(lz)], axis=1)
    basis = jnp.concatenate([defl_ref[0, 0, c] for c in range(lz)], axis=1)

    def halo_copies(k):
        field, car_x, car_y, car_z, bey_x, bey_y, bey_z, arr_xy, arr_z = ops[k]
        routes = (
            ("gx", -1, field, bey_x),
            ("gy", -1, field, bey_y),
            ("gz", -1, field.at[0], bey_z),
            ("gx", 1, car_x, arr_xy.at[0]),
            ("gy", 1, car_y, arr_xy.at[1]),
            ("gz", 1, car_z, arr_z),
        )
        copies = []
        for j, (axis, way, src, dst) in enumerate(routes):
            copies.append(
                (
                    lower[axis] if way < 0 else upper[axis],
                    upper[axis] if way < 0 else lower[axis],
                    pltpu.make_async_remote_copy(
                        src_ref=src,
                        dst_ref=dst,
                        send_sem=halo_send.at[k, j],
                        recv_sem=halo_recv.at[k, j],
                        device_id={axis: jnp.clip(idx[axis] + way, 0, sizes[axis] - 1)},
                        device_id_type=MESH,
                    ),
                )
            )
        return copies

    def start(copies):
        for sends, _, copy in copies:
            pl.when(sends)(copy.start)

    def open_product(k, v, later=None):
        field, car_x, car_y, car_z = ops[k][:4]
        copies = halo_copies(k) if later is None else None
        for c in range(lz):
            field[c] = v[:, span(c)]
        if later is None:
            start(copies[:3])
        for c in range(lz):
            carried = times(v[:, span(c)], out_h[c], out_l[c])
            car_x[c] = carried[:, span(0)]
            car_y[c] = carried[:, span(1)]
        car_z[...] = times(v[:, span(lz - 1)], zo_h[...], zo_l[...])
        if later is None:
            start(copies[3:])
        return times(v, loc_h[...], loc_l[...])

    def close_product(k, own):
        _, _, _, _, bey_x, bey_y, bey_z, arr_xy, arr_z = ops[k]
        for _, comes, copy in halo_copies(k):
            pl.when(comes)(copy.wait_recv)
        parts = []
        for c in range(lz):
            beyond = jnp.concatenate([bey_x[c], bey_y[c]], axis=1)
            part = times(beyond, in_h[c], in_l[c])
            part = part + arr_xy[0, c] + arr_xy[1, c]
            if c == 0:
                part = part + arr_z[...]
            if c == lz - 1:
                part = part + times(bey_z[...], zi_h[...], zi_l[...])
            parts.append(part)
        return own + jnp.concatenate(parts, axis=1)

    def gathered(buf, sem):
        rest = buf.at[pl.ds(0, buf.shape[0] - 1)]
        return pltpu.make_async_copy(rest, rest, sem)

    def reduce_start(buf, group, sem, value):
        me = position(group, sizes)
        buf[me] = value
        own = buf.at[me]

        def send(peer):
            pltpu.make_async_remote_copy(
                src_ref=own,
                dst_ref=own,
                send_sem=red_send.at[sem],
                recv_sem=red_recv.at[sem],
                device_id=peer,
                device_id_type=MESH,
            ).start()

        for_peers(group, sizes, send)

    def reduce_done(buf, sem):
        gathered(buf, red_recv.at[sem]).wait()
        return jnp.sum(buf[...], axis=0)

    def spread(coef, fields):
        return jnp.sum(coef * fields, axis=0, keepdims=True)

    rows_first = ops[0][0].shape[1]
    first = jnp.concatenate([basis, right, jnp.zeros((rows_first - defl - 1, lz * block), F32)], axis=0)
    pl.semaphore_wait(barrier, sum(extent(group, sizes) - 1 for group in COARSE_GROUPS))
    own = open_product(0, first)
    proj_h[...] = jnp.zeros_like(proj_h)
    proj_l[...] = jnp.zeros_like(proj_l)
    everything = slice(None)
    put(proj_h, proj_l, slice(0, defl), everything, basis)
    right_local = times_t(right, proj_h[...], proj_l[...])
    both = close_product(0, own)
    applied = both[:defl]
    image = both[defl : defl + 1]

    reps = block // defl
    apart = defl // reps
    for g in range(reps):
        put(proj_h, proj_l, slice(g * defl, (g + 1) * defl), everything, applied)
    coarse_local = times_t(basis, proj_h[...], proj_l[...])
    lane = lax.broadcasted_iota(jnp.int32, (apart, block), 1)
    packed = jnp.zeros((apart, block), F32)
    for g in range(reps):
        inside = (lane >= g * defl) & (lane < (g + 1) * defl)
        packed = packed + jnp.where(inside, coarse_local[g * apart : (g + 1) * apart], 0.0)
    sem = 0
    value = jnp.concatenate([packed, jnp.broadcast_to(right_local, (8, block))], axis=0)
    reduce_start(coarse_bufs[0], COARSE_GROUPS[0], sem, value)
    own = open_product(1, applied, "later")
    put(proj_h, proj_l, slice(defl, block), everything, jnp.zeros((block - defl, lz * block), F32))
    for k in range(1, len(COARSE_GROUPS)):
        value = reduce_done(coarse_bufs[k - 1], sem)
        sem += 1
        reduce_start(coarse_bufs[k], COARSE_GROUPS[k], sem, value)
    start(halo_copies(1))
    value = reduce_done(coarse_bufs[-1], sem)
    sem += 1
    coarse = jnp.concatenate(
        [value[:apart]] + [pltpu.roll(value[:apart], block - g * defl, 1) for g in range(1, reps)], axis=0
    )
    col = lax.broadcasted_iota(jnp.int32, (defl, block), 1)
    row = lax.broadcasted_iota(jnp.int32, (defl, block), 0)
    coarse = jnp.where(col < defl, coarse, 0.0)
    square = jnp.concatenate([coarse, jnp.zeros((block - defl, block), F32)], axis=0)
    inv = 0.5 * (coarse + square.T[:defl])
    for k in range(defl):
        pivot = 1.0 / inv[k : k + 1, k : k + 1]
        line = jnp.where(col[:1] == k, pivot, inv[k : k + 1] * pivot)
        inv = jnp.where(row == k, line, jnp.where(col == k, 0.0, inv) - inv[:, k : k + 1] * line)
    eye = jnp.where(row == col, 1.0, 0.0)

    def coarse_solve(projected):
        return jnp.sum(inv * projected, axis=1, keepdims=True)

    twice = close_product(1, own)
    coef = coarse_solve(value[apart : apart + 1])
    x = spread(coef, basis)
    r = right - spread(coef, applied)
    w = image - spread(coef, twice)
    d = s = z = curv = norm = None
    lane_row = lax.broadcasted_iota(jnp.int32, (1, block), 1)
    for it in range(ITERS):
        last = it + 1 == ITERS
        local = times_t(r, proj_h[...], proj_l[...])
        sq = jnp.sum(r * r, axis=1, keepdims=True)
        cross = jnp.sum(r * w, axis=1, keepdims=True)
        local = jnp.where(lane_row == defl, sq, jnp.where(lane_row == defl + 1, cross, local))
        bufs = dot_bufs[it]
        reduce_start(bufs[0], DOT_GROUPS[0], sem, local)
        if not last:
            own = open_product(2 + it, w)
        for k in range(1, len(DOT_GROUPS)):
            local = reduce_done(bufs[k - 1], sem)
            sem += 1
            reduce_start(bufs[k], DOT_GROUPS[k], sem, local)
        if not last:
            q = close_product(2 + it, own)
        total = reduce_done(bufs[-1], sem)
        sem += 1
        coef = coarse_solve(total)
        mine = jnp.sum(eye * total, axis=1, keepdims=True)
        energy = jnp.sum(mine * coef, axis=0, keepdims=True)
        norm_new = total[:, defl : defl + 1]
        cross = total[:, defl + 1 : defl + 2]
        if it == 0:
            d = r - spread(coef, basis)
            s = w - spread(coef, applied)
            z = q - spread(coef, twice)
            curv = cross - energy
        else:
            growth = norm_new / norm
            d = r + growth * d - spread(coef, basis)
            s = w + growth * s - spread(coef, applied)
            if not last:
                z = q + growth * z - spread(coef, twice)
            curv = cross - growth * growth * curv - energy
        norm = norm_new
        step = norm / curv
        x = x + step * d
        r = r - step * s
        if not last:
            w = w - step * z
    for c in range(lz):
        sol_ref[0, 0, c : c + 1, :] = x[:, span(c)]
        res_ref[0, 0, c : c + 1, :] = r[:, span(c)]

    for k in range(n_ops):
        for sends, _, copy in halo_copies(k):
            pl.when(sends)(copy.wait_send)
    every = list(coarse_bufs) + [buf for bufs in dot_bufs for buf in bufs]
    for k, buf in enumerate(every):
        gathered(buf, red_send.at[k]).wait()


def hand_out(sol_ref, res_ref, sol_out, res_out, sol_held, res_held, sems):
    def move(routes, k):
        copies = [pltpu.make_async_copy(src, dst, sems.at[k, j]) for j, (src, dst) in enumerate(routes)]
        for copy in copies:
            copy.start()
        for copy in copies:
            copy.wait()

    move(((sol_ref, sol_held), (res_ref, res_held)), 0)
    move(((sol_held, sol_out), (res_held, res_out)), 1)


def solution(mesh):
    sizes = dict(mesh.shape)
    in_specs = (
        P("gx", "gy", "gz", None),
        P("gx", "gy", "gz", None, None),
        P(None, "gx", "gy", "gz", None, None),
        P(None, "gx", "gy", "gz"),
        P("gx", "gy", "gz", None, None),
    )
    out_specs = (P("gx", "gy", "gz", None), P("gx", "gy", "gz", None))

    def per_device(right_side, diag_blocks, couplings, pattern, deflation):
        lx, ly, lz, block = right_side.shape
        pattern = jnp.transpose(pattern, (1, 2, 3, 0))
        assert lx == 1 and ly == 1
        defl = deflation.shape[3]
        rows_first = (defl + 1 + 7) // 8 * 8
        wide = lz * block
        scratch = []
        for shape in (
            (wide, wide),
            (lz, block, 2 * block),
            (lz, 2 * block, block),
            (block, block),
            (block, block),
            (block, wide),
        ):
            scratch += [pltpu.VMEM(shape, BF16)] * 2
        for rows in (rows_first, defl) + (1,) * (ITERS - 1):
            layer, face = (lz, rows, block), (rows, block)
            scratch += [pltpu.VMEM(layer, F32)] * 3 + [pltpu.VMEM(face, F32)]
            scratch += [pltpu.VMEM(layer, F32)] * 2 + [pltpu.VMEM(face, F32)]
            scratch += [pltpu.VMEM((2,) + layer, F32), pltpu.VMEM(face, F32)]
        for group in COARSE_GROUPS:
            scratch.append(pltpu.VMEM((extent(group, sizes), defl * defl // block + 8, block), F32))
        for _ in range(ITERS):
            for group in DOT_GROUPS:
                scratch.append(pltpu.VMEM((extent(group, sizes), 1, block), F32))
        reductions = len(COARSE_GROUPS) + ITERS * len(DOT_GROUPS)
        scratch += [pltpu.SemaphoreType.DMA((1 + ITERS, 6))] * 2
        scratch += [pltpu.SemaphoreType.DMA((reductions,))] * 2
        scratch.append(pltpu.SemaphoreType.DMA((5,)))
        for array in (right_side, diag_blocks, couplings, pattern, deflation):
            scratch.append(pltpu.VMEM(array.shape, array.dtype))
        vmem = pl.BlockSpec(memory_space=pltpu.VMEM)
        hbm = pl.BlockSpec(memory_space=pltpu.HBM)
        anywhere = pl.BlockSpec(memory_space=pl.ANY)
        out = jax.ShapeDtypeStruct(right_side.shape, F32)
        results = pl.pallas_call(
            functools.partial(kernel, sizes, lz, block, defl),
            out_shape=(out, out),
            in_specs=[hbm] * 5,
            out_specs=(vmem, vmem),
            scratch_shapes=scratch,
            compiler_params=pltpu.CompilerParams(
                collective_id=0, has_side_effects=True, vmem_limit_bytes=67_043_328
            ),
        )(right_side, diag_blocks, couplings, pattern, deflation)
        return pl.pallas_call(
            hand_out,
            out_shape=(out, out),
            in_specs=[anywhere, anywhere],
            out_specs=(hbm, hbm),
            scratch_shapes=[pltpu.VMEM(out.shape, F32)] * 2 + [pltpu.SemaphoreType.DMA((2, 2))],
            compiler_params=pltpu.CompilerParams(vmem_limit_bytes=67_043_328),
        )(*results)

    return jax.shard_map(
        per_device, mesh=mesh, in_specs=in_specs, out_specs=out_specs, check_vma=False
    )
```

```python
import functools
import math

import jax
import jax.numpy as jnp
from jax import lax
from jax.experimental import pallas as pl
from jax.experimental.pallas import tpu as pltpu
from jax.sharding import PartitionSpec as P

ITERS = 3
AXES = ("gx", "gy", "gz")
COARSE_GROUPS = (("gy", "gz"), ("gx",))
UNROLLED = 32
DOT_GROUPS = (("gx", "gy", "gz"),)
MESH = pl.DeviceIdType.MESH
F32 = jnp.float32
BF16 = jnp.bfloat16


def place(index, group, sizes):
    coords = {}
    for axis in reversed(group):
        coords[axis] = lax.rem(index, sizes[axis])
        index = lax.div(index, sizes[axis])
    return coords


def position(group, sizes):
    index = 0
    for axis in group:
        index = index * sizes[axis] + lax.axis_index(axis)
    return index


def extent(group, sizes):
    return math.prod(sizes[axis] for axis in group)


def for_peers(group, sizes, action):
    count = extent(group, sizes)
    me = position(group, sizes)

    def body(k, carry):
        action(place(lax.rem(me + k, count), group, sizes))
        return carry

    if count <= UNROLLED:
        for k in range(1, count):
            body(k, 0)
    else:
        lax.fori_loop(1, count, body, 0)


def split_rows(v):
    high = v.astype(BF16).astype(F32)
    rest = v - high
    middle = rest.astype(BF16).astype(F32)
    low = rest - middle
    if v.shape[0] == 1:
        row = lax.broadcasted_iota(jnp.int32, (8, v.shape[1]), 0)
        parts = jnp.where(row == 0, high, jnp.where(row == 1, middle, jnp.where(row == 2, low, 0.0)))
    else:
        parts = jnp.concatenate([high, middle, low], axis=0)
    return parts.astype(BF16)


def join_rows(out, rows):
    return out[:rows] + (out[rows : 2 * rows] + out[2 * rows : 3 * rows])


def split_pair(m):
    high = m.astype(BF16)
    return high, (m - high.astype(F32)).astype(BF16)


def times(v, high, low):
    parts = split_rows(v)
    out = jnp.dot(parts, high, preferred_element_type=F32)
    out = out + jnp.dot(parts, low, preferred_element_type=F32)
    return join_rows(out, v.shape[0])


def times_t(v, high, low):
    parts = split_rows(v)
    dims = (((1,), (1,)), ((), ()))
    out = lax.dot_general(parts, high, dims, preferred_element_type=F32)
    out = out + lax.dot_general(parts, low, dims, preferred_element_type=F32)
    return join_rows(out, v.shape[0])


def kernel(sizes, lz, block, defl, *refs):
    inputs = refs[:5]
    sol_ref, res_ref = refs[5:7]
    (loc_h, loc_l, out_h, out_l, in_h, in_l, zo_h, zo_l, zi_h, zi_l, proj_h, proj_l) = refs[7:19]
    n_ops = 1 + ITERS
    at = 19
    ops = []
    for _ in range(n_ops):
        ops.append(refs[at : at + 9])
        at += 9
    coarse_bufs = refs[at : at + len(COARSE_GROUPS)]
    at += len(COARSE_GROUPS)
    moment_bufs = refs[at : at + len(COARSE_GROUPS)]
    at += len(COARSE_GROUPS)
    dot_bufs = [refs[at + k * len(DOT_GROUPS) : at + (k + 1) * len(DOT_GROUPS)] for k in range(ITERS - 1)]
    at += (ITERS - 1) * len(DOT_GROUPS)
    halo_send, halo_recv, red_send, red_recv, load_sem = refs[at : at + 5]
    staged = refs[at + 5 : at + 10]
    loads = [pltpu.make_async_copy(src, dst, load_sem.at[k]) for k, (src, dst) in enumerate(zip(inputs, staged))]
    for load in loads:
        load.start()
    right_ref, diag_ref, coup_ref, pat_ref, defl_ref = staged

    idx = {axis: lax.axis_index(axis) for axis in AXES}
    lower = {axis: idx[axis] > 0 for axis in AXES}
    upper = {axis: idx[axis] < sizes[axis] - 1 for axis in AXES}
    barrier = pltpu.get_barrier_semaphore()

    for op in ops:
        for ref in op[4:9]:
            ref[...] = jnp.zeros_like(ref)
        op[3][...] = jnp.zeros_like(op[3])

    def greet(peer):
        pl.semaphore_signal(barrier, inc=1, device_id=peer, device_id_type=MESH)

    for group in COARSE_GROUPS:
        for_peers(group, sizes, greet)
    for load in loads:
        load.wait()

    def gate(d, c):
        return pat_ref[0, 0, c : c + 1, d : d + 1].astype(F32)

    def put(ref_h, ref_l, rows, cols, value):
        high, low = split_pair(value)
        ref_h[rows, cols] = high
        ref_l[rows, cols] = low

    def span(c):
        return slice(c * block, (c + 1) * block)

    if lz > 2:
        loc_h[...] = jnp.zeros_like(loc_h)
        loc_l[...] = jnp.zeros_like(loc_l)
    for c in range(lz):
        put(loc_h, loc_l, span(c), span(c), diag_ref[0, 0, c])
        cx = gate(0, c) * coup_ref[0, 0, 0, c]
        cy = gate(1, c) * coup_ref[1, 0, 0, c]
        cz = gate(2, c) * coup_ref[2, 0, 0, c]
        put(out_h.at[c], out_l.at[c], slice(None), span(0), cx)
        put(out_h.at[c], out_l.at[c], slice(None), span(1), cy)
        put(in_h.at[c], in_l.at[c], span(0), slice(None), cx.T)
        put(in_h.at[c], in_l.at[c], span(1), slice(None), cy.T)
        if c + 1 < lz:
            put(loc_h, loc_l, span(c), span(c + 1), cz)
            put(loc_h, loc_l, span(c + 1), span(c), cz.T)
        else:
            put(zo_h, zo_l, slice(None), slice(None), cz)
            put(zi_h, zi_l, slice(None), slice(None), cz.T)

    right = jnp.concatenate([right_ref[0, 0, c : c + 1, :] for c in range(lz)], axis=1)
    basis = jnp.concatenate([defl_ref[0, 0, c] for c in range(lz)], axis=1)

    def halo_copies(k):
        field, car_x, car_y, car_z, bey_x, bey_y, bey_z, arr_xy, arr_z = ops[k]
        routes = (
            ("gx", -1, field, bey_x),
            ("gy", -1, field, bey_y),
            ("gz", -1, field.at[0], bey_z),
            ("gx", 1, car_x, arr_xy.at[0]),
            ("gy", 1, car_y, arr_xy.at[1]),
            ("gz", 1, car_z, arr_z),
        )
        copies = []
        for j, (axis, way, src, dst) in enumerate(routes):
            copies.append(
                (
                    lower[axis] if way < 0 else upper[axis],
                    upper[axis] if way < 0 else lower[axis],
                    pltpu.make_async_remote_copy(
                        src_ref=src,
                        dst_ref=dst,
                        send_sem=halo_send.at[k, j],
                        recv_sem=halo_recv.at[k, j],
                        device_id={axis: jnp.clip(idx[axis] + way, 0, sizes[axis] - 1)},
                        device_id_type=MESH,
                    ),
                )
            )
        return copies

    def start(copies):
        for sends, _, copy in copies:
            pl.when(sends)(copy.start)

    def open_product(k, v, later=None):
        field, car_x, car_y, car_z = ops[k][:4]
        copies = halo_copies(k) if later is None else None
        for c in range(lz):
            field[c] = v[:, span(c)]
        if later is None:
            start(copies[:3])
        for c in range(lz):
            carried = times(v[:, span(c)], out_h[c], out_l[c])
            car_x[c] = carried[:, span(0)]
            car_y[c] = carried[:, span(1)]
        car_z[...] = times(v[:, span(lz - 1)], zo_h[...], zo_l[...])
        if later is None:
            start(copies[3:])
        return times(v, loc_h[...], loc_l[...])

    def close_product(k, own):
        _, _, _, _, bey_x, bey_y, bey_z, arr_xy, arr_z = ops[k]
        for _, comes, copy in halo_copies(k):
            pl.when(comes)(copy.wait_recv)
        parts = []
        for c in range(lz):
            beyond = jnp.concatenate([bey_x[c], bey_y[c]], axis=1)
            part = times(beyond, in_h[c], in_l[c])
            part = part + arr_xy[0, c] + arr_xy[1, c]
            if c == 0:
                part = part + arr_z[...]
            if c == lz - 1:
                part = part + times(bey_z[...], zi_h[...], zi_l[...])
            parts.append(part)
        return own + jnp.concatenate(parts, axis=1)

    def gathered(buf, sem):
        rest = buf.at[pl.ds(0, buf.shape[0] - 1)]
        return pltpu.make_async_copy(rest, rest, sem)

    def reduce_start(buf, group, sem, value):
        me = position(group, sizes)
        buf[me] = value
        own = buf.at[me]

        def send(peer):
            pltpu.make_async_remote_copy(
                src_ref=own,
                dst_ref=own,
                send_sem=red_send.at[sem],
                recv_sem=red_recv.at[sem],
                device_id=peer,
                device_id_type=MESH,
            ).start()

        for_peers(group, sizes, send)

    def reduce_done(buf, sem):
        gathered(buf, red_recv.at[sem]).wait()
        return jnp.sum(buf[...], axis=0)

    def spread(coef, fields):
        return jnp.sum(coef * fields, axis=0, keepdims=True)

    rows_first = ops[0][0].shape[1]
    first = jnp.concatenate([basis, right, jnp.zeros((rows_first - defl - 1, lz * block), F32)], axis=0)
    pl.semaphore_wait(barrier, sum(extent(group, sizes) - 1 for group in COARSE_GROUPS))
    own = open_product(0, first)
    proj_h[...] = jnp.zeros_like(proj_h)
    proj_l[...] = jnp.zeros_like(proj_l)
    everything = slice(None)
    put(proj_h, proj_l, slice(0, defl), everything, basis)
    right_local = times_t(right, proj_h[...], proj_l[...])
    both = close_product(0, own)
    applied = both[:defl]
    image = both[defl : defl + 1]

    reps = block // defl
    apart = defl // reps
    for g in range(reps):
        put(proj_h, proj_l, slice(g * defl, (g + 1) * defl), everything, applied)
    coarse_local = times_t(basis, proj_h[...], proj_l[...])
    lane = lax.broadcasted_iota(jnp.int32, (apart, block), 1)
    lane_row = lax.broadcasted_iota(jnp.int32, (1, block), 1)
    col = lax.broadcasted_iota(jnp.int32, (defl, block), 1)
    row = lax.broadcasted_iota(jnp.int32, (defl, block), 0)
    eye = jnp.where(row == col, 1.0, 0.0)

    def pack(repeated):
        packed = jnp.zeros((apart, block), F32)
        for g in range(reps):
            inside = (lane >= g * defl) & (lane < (g + 1) * defl)
            packed = packed + jnp.where(inside, repeated[g * apart : (g + 1) * apart], 0.0)
        return packed

    def unpack(packed):
        groups = [packed] + [pltpu.roll(packed, block - g * defl, 1) for g in range(1, reps)]
        return jnp.where(col < defl, jnp.concatenate(groups, axis=0), 0.0)

    def on_applied(v):
        return times_t(v, proj_h[...], proj_l[...])

    stages = len(COARSE_GROUPS)
    value = jnp.concatenate([pack(coarse_local), jnp.broadcast_to(right_local, (8, block))], axis=0)
    reduce_start(coarse_bufs[0], COARSE_GROUPS[0], 0, value)
    own = open_product(1, both)
    second = pack(on_applied(applied))
    h_right, h_image = on_applied(right), on_applied(image)
    sq = jnp.sum(right * right, axis=1, keepdims=True)
    cross = jnp.sum(right * image, axis=1, keepdims=True)
    h_right = jnp.where(lane_row == defl, sq, jnp.where(lane_row == defl + 1, cross, h_right))
    row8 = lax.broadcasted_iota(jnp.int32, (8, block), 0)
    vectors = jnp.where(row8 == 0, h_right, h_image)
    for k in range(1, stages):
        value = reduce_done(coarse_bufs[k - 1], k - 1)
        reduce_start(coarse_bufs[k], COARSE_GROUPS[k], k, value)
    both_twice = close_product(1, own)
    twice = both_twice[:defl]
    image_twice = both_twice[defl : defl + 1]
    moments = jnp.concatenate([second, pack(on_applied(twice)), vectors], axis=0)
    reduce_start(moment_bufs[0], COARSE_GROUPS[0], stages, moments)
    own = open_product(2, twice, "later")
    value = reduce_done(coarse_bufs[-1], stages - 1)
    coarse = unpack(value[:apart])
    square = jnp.concatenate([coarse, jnp.zeros((block - defl, block), F32)], axis=0)
    inv = 0.5 * (coarse + square.T[:defl])
    for k in range(defl):
        if k == defl // 2:
            for j in range(1, stages):
                moments = reduce_done(moment_bufs[j - 1], stages + j - 1)
                reduce_start(moment_bufs[j], COARSE_GROUPS[j], stages + j, moments)
            start(halo_copies(2))
        pivot = 1.0 / inv[k : k + 1, k : k + 1]
        line = jnp.where(col[:1] == k, pivot, inv[k : k + 1] * pivot)
        inv = jnp.where(row == k, line, jnp.where(col == k, 0.0, inv) - inv[:, k : k + 1] * line)

    def coarse_solve(projected):
        return jnp.sum(inv * projected, axis=1, keepdims=True)

    coef = coarse_solve(value[apart : apart + 1])
    coef_row = spread(coef, eye)
    x = spread(coef, basis)
    r = right - spread(coef, applied)
    w = image - spread(coef, twice)
    moments = reduce_done(moment_bufs[-1], 2 * stages - 1)
    h_right = moments[2 * apart : 2 * apart + 1]
    h_image = moments[2 * apart + 1 : 2 * apart + 2]
    onto = spread(coef, unpack(moments[:apart]))
    onto_image = spread(coef, unpack(moments[apart : 2 * apart]))
    sq = h_right[:, defl : defl + 1] + jnp.sum(coef_row * (onto - 2.0 * h_right), axis=1, keepdims=True)
    cross = h_right[:, defl + 1 : defl + 2] + jnp.sum(coef_row * (onto_image - 2.0 * h_image), axis=1, keepdims=True)
    total = jnp.where(lane_row == defl, sq, jnp.where(lane_row == defl + 1, cross, h_right - onto))
    q = image_twice - spread(coef, close_product(2, own))
    d = s = z = curv = norm = None
    sem = 2 * stages
    for it in range(ITERS):
        last = it + 1 == ITERS
        if it > 0:
            local = on_applied(r)
            sq = jnp.sum(r * r, axis=1, keepdims=True)
            cross = jnp.sum(r * w, axis=1, keepdims=True)
            local = jnp.where(lane_row == defl, sq, jnp.where(lane_row == defl + 1, cross, local))
            bufs = dot_bufs[it - 1]
            reduce_start(bufs[0], DOT_GROUPS[0], sem, local)
            if not last:
                own = open_product(2 + it, w)
            for k in range(1, len(DOT_GROUPS)):
                local = reduce_done(bufs[k - 1], sem)
                sem += 1
                reduce_start(bufs[k], DOT_GROUPS[k], sem, local)
            if not last:
                q = close_product(2 + it, own)
            total = reduce_done(bufs[-1], sem)
            sem += 1
        coef = coarse_solve(total)
        mine = jnp.sum(eye * total, axis=1, keepdims=True)
        energy = jnp.sum(mine * coef, axis=0, keepdims=True)
        norm_new = total[:, defl : defl + 1]
        cross = total[:, defl + 1 : defl + 2]
        if it == 0:
            d = r - spread(coef, basis)
            s = w - spread(coef, applied)
            z = q - spread(coef, twice)
            curv = cross - energy
        else:
            growth = norm_new / norm
            d = r + growth * d - spread(coef, basis)
            s = w + growth * s - spread(coef, applied)
            if not last:
                z = q + growth * z - spread(coef, twice)
            curv = cross - growth * growth * curv - energy
        norm = norm_new
        step = norm / curv
        x = x + step * d
        r = r - step * s
        if not last:
            w = w - step * z
    for c in range(lz):
        sol_ref[0, 0, c : c + 1, :] = x[:, span(c)]
        res_ref[0, 0, c : c + 1, :] = r[:, span(c)]

    for k in range(n_ops):
        for sends, _, copy in halo_copies(k):
            pl.when(sends)(copy.wait_send)
    every = list(coarse_bufs) + list(moment_bufs) + [buf for bufs in dot_bufs for buf in bufs]
    for k, buf in enumerate(every):
        gathered(buf, red_send.at[k]).wait()


def hand_out(sol_ref, res_ref, sol_out, res_out, sol_held, res_held, sems):
    def move(routes, k):
        copies = [pltpu.make_async_copy(src, dst, sems.at[k, j]) for j, (src, dst) in enumerate(routes)]
        for copy in copies:
            copy.start()
        for copy in copies:
            copy.wait()

    move(((sol_ref, sol_held), (res_ref, res_held)), 0)
    move(((sol_held, sol_out), (res_held, res_out)), 1)


def solution(mesh):
    sizes = dict(mesh.shape)
    in_specs = (
        P("gx", "gy", "gz", None),
        P("gx", "gy", "gz", None, None),
        P(None, "gx", "gy", "gz", None, None),
        P(None, "gx", "gy", "gz"),
        P("gx", "gy", "gz", None, None),
    )
    out_specs = (P("gx", "gy", "gz", None), P("gx", "gy", "gz", None))

    def per_device(right_side, diag_blocks, couplings, pattern, deflation):
        lx, ly, lz, block = right_side.shape
        pattern = jnp.transpose(pattern, (1, 2, 3, 0))
        assert lx == 1 and ly == 1
        defl = deflation.shape[3]
        rows_first = (defl + 1 + 7) // 8 * 8
        wide = lz * block
        scratch = []
        for shape in (
            (wide, wide),
            (lz, block, 2 * block),
            (lz, 2 * block, block),
            (block, block),
            (block, block),
            (block, wide),
        ):
            scratch += [pltpu.VMEM(shape, BF16)] * 2
        for rows in (rows_first, rows_first, defl) + (1,) * (ITERS - 2):
            layer, face = (lz, rows, block), (rows, block)
            scratch += [pltpu.VMEM(layer, F32)] * 3 + [pltpu.VMEM(face, F32)]
            scratch += [pltpu.VMEM(layer, F32)] * 2 + [pltpu.VMEM(face, F32)]
            scratch += [pltpu.VMEM((2,) + layer, F32), pltpu.VMEM(face, F32)]
        for group in COARSE_GROUPS:
            scratch.append(pltpu.VMEM((extent(group, sizes), defl * defl // block + 8, block), F32))
        for group in COARSE_GROUPS:
            scratch.append(pltpu.VMEM((extent(group, sizes), 2 * defl * defl // block + 8, block), F32))
        for _ in range(ITERS - 1):
            for group in DOT_GROUPS:
                scratch.append(pltpu.VMEM((extent(group, sizes), 1, block), F32))
        reductions = 2 * len(COARSE_GROUPS) + (ITERS - 1) * len(DOT_GROUPS)
        scratch += [pltpu.SemaphoreType.DMA((1 + ITERS, 6))] * 2
        scratch += [pltpu.SemaphoreType.DMA((reductions,))] * 2
        scratch.append(pltpu.SemaphoreType.DMA((5,)))
        for array in (right_side, diag_blocks, couplings, pattern, deflation):
            scratch.append(pltpu.VMEM(array.shape, array.dtype))
        vmem = pl.BlockSpec(memory_space=pltpu.VMEM)
        hbm = pl.BlockSpec(memory_space=pltpu.HBM)
        anywhere = pl.BlockSpec(memory_space=pl.ANY)
        out = jax.ShapeDtypeStruct(right_side.shape, F32)
        results = pl.pallas_call(
            functools.partial(kernel, sizes, lz, block, defl),
            out_shape=(out, out),
            in_specs=[hbm] * 5,
            out_specs=(vmem, vmem),
            scratch_shapes=scratch,
            compiler_params=pltpu.CompilerParams(
                collective_id=0, has_side_effects=True, vmem_limit_bytes=67_043_328
            ),
        )(right_side, diag_blocks, couplings, pattern, deflation)
        return pl.pallas_call(
            hand_out,
            out_shape=(out, out),
            in_specs=[anywhere, anywhere],
            out_specs=(hbm, hbm),
            scratch_shapes=[pltpu.VMEM(out.shape, F32)] * 2 + [pltpu.SemaphoreType.DMA((2, 2))],
            compiler_params=pltpu.CompilerParams(vmem_limit_bytes=67_043_328),
        )(*results)

    return jax.shard_map(
        per_device, mesh=mesh, in_specs=in_specs, out_specs=out_specs, check_vma=False
    )
```
